32 devices in a mesh: row: 8 (over z, y), col: 4 (over x, core).
Axes of the slice: x: 2, y: 2, z: 4, core: 2. Of those that a mesh axis runs over, the one named last changes fastest.
Arguments:
- matrix: float32 [4, 8, 512, 8, 4, 512], P(None, 'row', None, None, 'col'), may hold values from -30 to 30, as said below
Outputs:
- factored: float32 [4, 8, 512, 8, 4, 512], P(None, 'row', None, None, 'col')
The draws below stay inside these ranges and needn't reach their ends.
Inputs may be any that keep to these rules, and one draw needn't show every extreme that they name: matrix is symmetric, positive definite and well conditioned.
All inputs are finite; a program needn't handle non-finite values.
Results may differ from the reference program's by a relative error of at most 0.00013.
Values sent between devices are 32-bit elements; how exact they have to be, the bound alone decides.
A program may use at most 192 MiB of HBM per device.

```python
import jax
import jax.numpy as jnp
from jax import lax

N = 16384
NB = 512
STEPS = 2
TRL = 4
TCL = 8
N_ROW = 8
N_COL = 4


def draw_matrix(key, part):
    gram_cols = 2 * NB
    factor_scale = 2.0 / gram_cols ** 0.5
    key_factor = jax.random.fold_in(key, 11)
    key_diag = jax.random.fold_in(key, 12)
    factor_cols = jax.random.normal(key_factor, (N, gram_cols), jnp.float32) * factor_scale
    diag_values = jax.random.uniform(key_diag, (N,), jnp.float32, 1.0, 2.0)
    scaling = jnp.ones((N,), jnp.float32)
    square = jnp.dot(factor_cols, factor_cols.T, precision=lax.Precision.HIGHEST, preferred_element_type=jnp.float32)
    square = 0.5 * (square + square.T) + jnp.diag(diag_values)
    square = scaling[:, None] * square * scaling[None, :]
    return square.reshape(TRL, N_ROW, NB, TCL, N_COL, NB).astype(jnp.float32)


def setup_inputs(seed: int = 0) -> dict:
    keys = jax.random.split(jax.random.key(seed), 2)
    return {
        "matrix": draw_matrix(jax.random.fold_in(keys[1], 71), 0),
    }


def reference(matrix):
    square = matrix.reshape(N, N)
    for step in range(STEPS):
        begin_at = step * NB
        end_at = begin_at + NB
        diag_factor = jnp.linalg.cholesky(square[begin_at:end_at, begin_at:end_at])
        lower_part = square[end_at:, begin_at:end_at]
        column_panel = jax.scipy.linalg.solve_triangular(diag_factor, lower_part.T, lower=True).T
        trailing = square[end_at:, end_at:] - jnp.dot(column_panel.astype(jnp.float32), column_panel.T.astype(jnp.float32), precision=lax.Precision.HIGHEST, preferred_element_type=jnp.float32)
        square = square.at[end_at:, end_at:].set(trailing)
        square = square.at[end_at:, begin_at:end_at].set(column_panel)
        square = square.at[begin_at:end_at, begin_at:end_at].set(diag_factor)
        square = square.at[begin_at:end_at, end_at:].set(jnp.zeros((NB, N - end_at), jnp.float32))
    return square.reshape(matrix.shape)
```

```python
import jax
import jax.numpy as jnp
from jax import lax
from jax.experimental import pallas as pl
from jax.experimental.pallas import tpu as pltpu
from jax.sharding import PartitionSpec as P

NB = 512
STEPS = 2
HIGHEST = lax.Precision.HIGHEST
LANES = 128


def dot_nt(a, b, precision):
    return lax.dot_general(
        a, b, (((1,), (1,)), ((), ())), precision=precision, preferred_element_type=jnp.float32
    )


def factor_tile(work, factor, inverse, pair):
    size = work.shape[0]
    sub = lax.broadcasted_iota(jnp.int32, (LANES, LANES), 0)
    lane = lax.broadcasted_iota(jnp.int32, (LANES, LANES), 1)
    sub_wide = lax.broadcasted_iota(jnp.int32, (LANES, 2 * LANES), 0)
    lane_wide = lax.broadcasted_iota(jnp.int32, (1, 2 * LANES), 1)
    factor[...] = jnp.zeros_like(factor)
    inverse[...] = jnp.zeros_like(inverse)
    for begin in range(0, size, LANES):
        end = begin + LANES
        here = slice(begin, end)
        pair[:, :LANES] = work[here, here]
        pair[:, LANES:] = jnp.where(sub == lane, 1.0, 0.0)

        def eliminate(j, carry):
            row = pair[pl.ds(j, 1), :]
            pivot = jnp.sum(jnp.where(lane_wide == j, row, 0.0), axis=1, keepdims=True)
            scale = 1.0 / jnp.sqrt(pivot)
            row = row * scale
            now = pair[...]
            column = jnp.sum(jnp.where(lane == j, now[:, :LANES], 0.0), axis=1, keepdims=True)
            column = column * scale
            pair[...] = jnp.where(
                sub_wide > j, now - column * row, jnp.where(sub_wide == j, row, now)
            )
            return carry

        lax.fori_loop(0, LANES, eliminate, 0)
        factor[here, here] = jnp.where(sub <= lane, pair[:, :LANES], 0.0).T
        small = jnp.where(sub >= lane, pair[:, LANES:], 0.0)
        if end < size:
            panel = dot_nt(work[end:, here], small, HIGHEST)
            factor[end:, here] = panel
            work[end:, end:] = work[end:, end:] - dot_nt(panel, panel, HIGHEST)
        inverse[here, here] = small
        if begin:
            known = jnp.dot(factor[here, :begin], inverse[:begin, :begin], precision=HIGHEST)
            inverse[here, :begin] = -jnp.dot(small, known, precision=HIGHEST)


def factor_kernel(lead, factor_0, inverse_0, below, factor_1, inverse_1, work, pair):
    work[...] = lead[0]
    factor_tile(work, factor_0, inverse_0, pair)
    solved = dot_nt(lead[1], inverse_0[...], HIGHEST)
    below[...] = solved
    work[...] = lead[2] - dot_nt(solved, solved, HIGHEST)
    factor_tile(work, factor_1, inverse_1, pair)


def factor_lead(lead):
    tile = jax.ShapeDtypeStruct((NB, NB), jnp.float32)
    return pl.pallas_call(
        factor_kernel,
        out_shape=[tile] * 5,
        in_specs=[pl.BlockSpec(memory_space=pltpu.VMEM)],
        out_specs=[pl.BlockSpec(memory_space=pltpu.VMEM)] * 5,
        scratch_shapes=[
            pltpu.VMEM((NB, NB), jnp.float32),
            pltpu.VMEM((LANES, 2 * LANES), jnp.float32),
        ],
        cost_estimate=pl.CostEstimate(flops=10**11, bytes_accessed=10**7, transcendentals=0),
        name="factor_lead",
    )(lead)


def update_kernel(column_count, place, x, row_high, row_low, col_high, col_low, fresh, out):
    rows = row_high.shape[0]
    stride = x.shape[0] // rows
    local_cols = col_high.shape[0] // NB
    p, q = place[0], place[1]
    lead_rows = (pl.program_id(0) * rows < NB) & (p < STEPS)
    high, low = row_high[...], row_low[...]
    for s in range(local_cols):
        tile = slice(s * NB, (s + 1) * NB)
        product = dot_nt(high, col_high[tile, :], None)
        product += dot_nt(high, col_low[tile, :], None)
        product += dot_nt(low, col_high[tile, :], None)
        clear = lead_rows & (s * column_count + q > p)
        for c in range(NB // LANES):
            part = slice(c * LANES, (c + 1) * LANES)
            at = pl.ds(s * (NB // LANES) + c, rows, stride=stride)
            value = x[at, :] - product[:, part]
            if s == 0:
                value = jnp.where(q < STEPS, fresh[:, part], value)
            out[at, :] = jnp.where(clear, 0.0, value)


def split(x):
    high = lax.reduce_precision(x, 8, 7)
    return high.astype(jnp.bfloat16), (x - high).astype(jnp.bfloat16)


def update(place, matrix, row_panel, column_panel, fresh, column_count):
    rows, depth = row_panel.shape
    columns = column_panel.shape[0]
    chunk = 256
    lines = columns // LANES
    flat = matrix.reshape(rows * lines, LANES)
    row_high, row_low = split(row_panel)
    col_high, col_low = split(column_panel)
    whole = pl.BlockSpec((columns, depth), lambda i, _: (0, 0), pipeline_mode=pl.Buffered(1))
    part = pl.BlockSpec((chunk, depth), lambda i, _: (i, 0))
    line_block = pl.BlockSpec((chunk * lines, LANES), lambda i, _: (i, 0))
    out = pl.pallas_call(
        lambda *refs: update_kernel(column_count, *refs),
        out_shape=jax.ShapeDtypeStruct(flat.shape, jnp.float32),
        grid_spec=pltpu.PrefetchScalarGridSpec(
            num_scalar_prefetch=1,
            grid=(rows // chunk,),
            in_specs=[
                line_block, part, part, whole, whole, pl.BlockSpec((chunk, NB), lambda i, _: (i, 0))
            ],
            out_specs=line_block,
        ),
        compiler_params=pltpu.CompilerParams(vmem_limit_bytes=60 * 2**20),
        name="update",
    )(place, flat, row_high, row_low, col_high, col_low, fresh)
    return out.reshape(matrix.shape)


def shards(matrix):
    local_rows = matrix.shape[0]
    local_cols = matrix.shape[3]
    rows = local_rows * NB
    lines = matrix.reshape(rows, local_cols * NB // LANES, LANES)
    mine = lax.optimization_barrier(lines)[:, : NB // LANES].reshape(rows, NB)
    row_count = lax.axis_size("row")
    column_count = lax.axis_size("col")
    group_size = row_count // column_count
    row_place = lax.axis_index("row")
    column_place = lax.axis_index("col")
    tile_rows = jnp.arange(local_rows, dtype=jnp.int32) * row_count + row_place

    corner = mine[:NB]
    at = lambda p, q: (row_place == p) & (column_place == q)
    lead = jnp.stack([jnp.where(at(p, q), corner, 0.0) for p, q in ((0, 0), (1, 0), (1, 1))])
    lead = lax.psum(lead, ("row", "col"))

    swapped = lax.ppermute(mine, "col", [(0, 1), (1, 0)])
    crossed = lax.ppermute(mine, "col", [(0, 2), (1, 3)])
    partner = lax.ppermute(crossed, "col", [(2, 3), (3, 2)])
    near = column_place < 2
    own_half = jnp.where(near, mine, crossed)
    other_half = jnp.where(near, swapped, partner)
    even = column_place % 2 == 0
    raw = jnp.concatenate(
        [jnp.where(even, own_half, other_half), jnp.where(even, other_half, own_half)], axis=1
    )

    pieces = raw.reshape(column_count, rows // column_count, 2 * NB)
    part = row_place % column_count
    piece = lax.dynamic_index_in_dim(pieces, part, 0, keepdims=False)
    for shift in range(1, column_count):
        pairs = [
            (
                (h * column_count + q) * column_count + q,
                (h * column_count + (q + shift) % column_count) * column_count + q,
            )
            for h in range(group_size)
            for q in range(column_count)
        ]
        send = lax.dynamic_index_in_dim(
            pieces, (column_place + shift) % column_count, 0, keepdims=False
        )
        got = lax.ppermute(send, ("row", "col"), pairs)
        piece = jnp.where(part == (column_place + shift) % column_count, got, piece)
    gathered = lax.all_gather(piece, "row", axis=0)

    factor_0, inverse_0, below, factor_1, inverse_1 = factor_lead(lead)

    def solve(panel):
        first = dot_nt(panel[:, :NB], inverse_0, HIGHEST)
        rest = panel[:, NB:] - dot_nt(first, below, HIGHEST)
        return first, dot_nt(rest, inverse_1, HIGHEST)

    first, second = (x.reshape(local_rows, NB, NB) for x in solve(raw))
    row_id = tile_rows[:, None, None]
    column_0 = jnp.where(row_id == 0, factor_0, first)
    column_1 = jnp.where(row_id == 0, 0.0, jnp.where(row_id == 1, factor_1, second))
    row_panel = jnp.concatenate([first, second], axis=2).reshape(rows, 2 * NB)
    fresh = jnp.where(column_place == 0, column_0, column_1).reshape(rows, NB)

    ordered = gathered.reshape(group_size, local_rows, NB, 2 * NB).transpose(1, 0, 2, 3)
    column_panel = jnp.concatenate(solve(ordered.reshape(local_cols * NB, 2 * NB)), axis=1)
    place = jnp.stack([row_place, column_place]).astype(jnp.int32)
    return update(place, lines, row_panel, column_panel, fresh, column_count).reshape(matrix.shape)


def solution(mesh):
    in_specs = (P(None, "row", None, None, "col", None),)
    out_specs = P(None, "row", None, None, "col", None)
    return jax.shard_map(shards, mesh=mesh, in_specs=in_specs, out_specs=out_specs, check_vma=False)
```
